32 devices in a mesh: rows: 8 (over z, x), grid: 4 (over y, core).
Axes of the slice: x: 2, y: 2, z: 4, core: 2. Of those that a mesh axis runs over, the one named last changes fastest.
Arguments:
- design: bfloat16 [98304, 1024], P(('rows', 'grid')), may hold values from -6 to 6
- observed: float32 [98304], P(('rows', 'grid')), may hold values from -6 to 6
- weight_class: int32 [98304], P(('rows', 'grid')), may hold values from 0 to 15
- calib_unit: int32 [98304], P(('rows', 'grid')), may hold values from 0 to 63
- class_weight: float32 [16], replicated, may hold values from 0.5 to 8
- calib_scale: float32 [64, 8], replicated, may hold values from 0.5 to 2
Outputs:
- normal_matrix: float32 [1024, 1024], P('rows', 'grid')
- right_hand: float32 [1024], P(('rows', 'grid'))
- chi_square: float32 [], replicated
The draws below stay inside these ranges and needn't reach their ends.
All inputs are finite; a program needn't handle non-finite values.
Results may differ from the reference program's by a relative error of at most 0.01.
Values sent between devices are 32-bit elements; how exact they have to be, the bound alone decides.
A program may use at most 64 MiB of HBM per device.

```python
import math
import jax
import jax.numpy as jnp
from jax import lax

P_SIZE = 1024
CB = 128
NB = 8
UNITS = 64
CLASSES = 16
ROW_DEV = 3072
NROWS = 98304


def set_ends(result, own_key, low, high):
    index_at = [jax.random.randint(jax.random.fold_in(own_key, axis), (), 0, length) for axis, length in enumerate(result.shape)]
    longest = result.shape.index(max(result.shape))
    neighbour = index_at[:longest] + [(index_at[longest] + 1) % result.shape[longest]] + index_at[longest + 1:]
    return result.at[tuple(index_at)].set(low).at[tuple(neighbour)].set(high)


def strengthened(array, rng, source, target, blocks, factor):
    owner, partner = [(jnp.arange(array.shape[dim]) // (array.shape[dim] // blocks)).reshape([-1 if axis == dim else 1 for axis in range(array.ndim)]) for dim in (source, target)]
    chosen = jax.random.permutation(rng, blocks)[partner]
    strong = (owner == chosen) | (owner == (partner + blocks // 2) % blocks)
    return jnp.where(strong, factor * array, array)


def block_scale(key, shape, pieces, least, largest):
    gain = 1.0
    for dim, shards_of in pieces:
        steps = jax.random.uniform(jax.random.fold_in(jax.random.fold_in(key, 6), dim), (shards_of,), jnp.float32, least / len(pieces), largest / len(pieces))
        gain = gain * jnp.repeat(jnp.exp(steps), shape[dim] // shards_of).reshape((-1,) + (1,) * (len(shape) - 1 - dim))
    return gain


def normal_values(own_key, dims, scale, reach, cuts=(), dtype=jnp.bfloat16):
    level = block_scale(own_key, dims, cuts, -0.22, 0.18) if cuts else 1.0
    result = jax.random.normal(own_key, dims, jnp.float32) * scale * level
    return jnp.minimum(jnp.maximum(result, -reach), reach).astype(dtype)


def heavy_noise(stream_key, dims, scale, limit, cuts, heavy, dtype=jnp.bfloat16):
    values = scale * jax.random.normal(stream_key, dims, jnp.float32)
    if cuts:
        values = values * block_scale(stream_key, dims, cuts, -0.22, 0.18)
    return jnp.clip(strengthened(values, jax.random.fold_in(stream_key, 3), *heavy), -limit, limit).astype(dtype)


def setup_inputs(seed: int = 0) -> dict:
    key_of = jax.random.split(jax.random.key(seed), 7)
    design = heavy_noise(key_of[0], (NROWS, P_SIZE), 1.0, 6.0, ((0, 32),), (0, 1, 32, 2.75))
    observed = normal_values(key_of[1], (NROWS,), 1.0, 6.0, ((0, 32),), jnp.float32)
    weight_class = set_ends(jax.random.randint(key_of[2], (NROWS,), 0, CLASSES), jax.random.fold_in(key_of[2], 1), 0, CLASSES - 1).astype(jnp.int32)
    calib_unit = set_ends(jax.random.randint(key_of[3], (NROWS,), 0, UNITS), jax.random.fold_in(key_of[3], 1), 0, UNITS - 1).astype(jnp.int32)
    class_weight = jnp.clip(jnp.exp(jax.random.uniform(key_of[4], (CLASSES,), jnp.float32, math.log(0.5), math.log(8.0))), 0.5, 8.0)
    calib_scale = jnp.clip(jnp.exp(jax.random.uniform(key_of[5], (UNITS, NB), jnp.float32, math.log(0.5), math.log(2.0))), 0.5, 2.0)
    return dict(design=design, observed=observed, weight_class=weight_class, calib_unit=calib_unit, class_weight=class_weight, calib_scale=calib_scale)


def reference(design, observed, weight_class, calib_unit, class_weight, calib_scale):
    shards = NROWS // ROW_DEV
    design_b = design.reshape(shards, ROW_DEV, P_SIZE)
    observed_b = observed.reshape(shards, ROW_DEV)
    class_b = weight_class.reshape(shards, ROW_DEV)
    unit_b = calib_unit.reshape(shards, ROW_DEV)

    def step(carry, items):
        gram, rhs, chi = carry
        block, obs, cls, unit = items
        row_weight = class_weight[cls]
        root_weight = jnp.sqrt(row_weight)
        scales = jnp.repeat(calib_scale[unit], CB, axis=1)
        scaled = (block.astype(jnp.float32) * scales).astype(jnp.bfloat16)
        weighted = (root_weight[:, None] * scaled.astype(jnp.float32)).astype(jnp.bfloat16)
        gram = gram + lax.dot_general(weighted, weighted, (((0,), (0,)), ((), ())), preferred_element_type=jnp.float32)
        weighted_obs = (root_weight * obs).astype(jnp.bfloat16)
        rhs = rhs + jnp.dot(weighted_obs, weighted, preferred_element_type=jnp.float32)
        chi = chi + jnp.sum(row_weight * obs * obs)
        return ((gram, rhs, chi), None)
    init = (jnp.zeros((P_SIZE, P_SIZE), jnp.float32), jnp.zeros((P_SIZE,), jnp.float32), jnp.zeros((), jnp.float32))
    (gram, rhs, chi), unused = lax.scan(step, init, (design_b, observed_b, class_b, unit_b))
    return (gram / NROWS, rhs / NROWS, chi / NROWS)
```

```python
import functools

import jax
import jax.numpy as jnp
from jax import lax
from jax.experimental import pallas as pl
from jax.experimental.pallas import tpu as pltpu
from jax.sharding import PartitionSpec as P

MESH = pl.DeviceIdType.MESH
LANES = 128
F32 = jnp.float32
BF16 = jnp.bfloat16


def plain(design, observed, weight_class, calib_unit, class_weight, calib_scale):
    row_count, width = design.shape
    blocks = calib_scale.shape[1]
    total_rows = row_count * lax.axis_size("rows") * lax.axis_size("grid")
    class_hot = (
        weight_class[:, None] == jnp.arange(class_weight.shape[0], dtype=jnp.int32)[None, :]
    ).astype(F32)
    row_weight = jnp.dot(class_hot, class_weight, precision=lax.Precision.HIGHEST)
    root_weight = jnp.sqrt(row_weight)
    unit_hot = (
        calib_unit[:, None] == jnp.arange(calib_scale.shape[0], dtype=jnp.int32)[None, :]
    ).astype(F32)
    row_scales = jnp.dot(unit_hot, calib_scale, precision=lax.Precision.HIGHEST)
    scaled = (
        (design.reshape(row_count, blocks, width // blocks).astype(F32) * row_scales[:, :, None])
        .reshape(row_count, width)
        .astype(BF16)
    )
    weighted = (root_weight[:, None] * scaled.astype(F32)).astype(BF16)
    term = lax.dot_general(weighted, weighted, (((0,), (0,)), ((), ())), preferred_element_type=F32)
    columns = lax.psum_scatter(term, "grid", scatter_dimension=1, tiled=True)
    gram = lax.psum_scatter(columns, "rows", scatter_dimension=0, tiled=True)
    weighted_obs = (root_weight * observed).astype(BF16)
    rhs_term = jnp.dot(weighted_obs, weighted, preferred_element_type=F32)
    chi_term = jnp.sum(row_weight * observed * observed)
    right_hand = lax.psum_scatter(rhs_term, ("rows", "grid"), scatter_dimension=0, tiled=True)
    chi_total = lax.psum(chi_term, ("rows", "grid"))
    return (gram / total_rows, right_hand / total_rows, chi_total / total_rows)


def split3(value):
    high = value.astype(BF16)
    rest = value - high.astype(F32)
    middle = rest.astype(BF16)
    low = (rest - middle.astype(F32)).astype(BF16)
    return high, middle, low


def kernel(
    dims,
    design_hbm, obs_ref, class_ref, unit_ref, cw_ref, cs_ref,
    gram_ref, aux_ref,
    raw, weighted, table, cwcol, rhs_acc, chi_acc,
    buf, rx0, s1, rx1, s2, rx2, s3, rx3, fin, ext, mrx, erx, axs, rxa,
    in_sem, q0, r0, q1, r1, q2, r2, q3, r3, qm, rm, qe, re, qa, ra,
):
    n_rows, n_grid, total_rows = dims
    n_z = n_rows // 2
    row_count, width = raw.shape
    units = cs_ref.shape[0]
    blocks = cs_ref.shape[1]
    classes = cw_ref.shape[0]
    half = LANES // 2
    piece = LANES // (2 * n_grid)
    sub = piece // 2
    r = lax.axis_index("rows")
    g = lax.axis_index("grid")
    z = r // 2
    x = lax.rem(r, 2)
    y = g // 2
    c = lax.rem(g, 2)
    me = r * n_grid + g
    count = n_rows * n_grid

    n_chunks = in_sem.shape[0]
    chunk = row_count // n_chunks
    loads = [
        pltpu.make_async_copy(
            design_hbm.at[pl.ds(k * chunk, chunk)], raw.at[pl.ds(k * chunk, chunk)], in_sem.at[k]
        )
        for k in range(n_chunks)
    ]
    for load in loads:
        load.start()

    barrier = pltpu.get_barrier_semaphore()

    def greet(k, carry):
        flat = lax.rem(me + k, count)
        pl.semaphore_signal(
            barrier, inc=1, device_id=(flat // n_grid, lax.rem(flat, n_grid)), device_id_type=MESH
        )
        return carry

    lax.fori_loop(1, count, greet, 0)

    depth = table.shape[0]
    table[...] = jnp.zeros_like(table)
    for b in range(blocks):
        wide = jnp.broadcast_to(cs_ref[:, b : b + 1], (units, LANES))
        for t, term in enumerate(split3(wide)):
            table[t * units : (t + 1) * units, b * LANES : (b + 1) * LANES] = term
    index = lax.broadcasted_iota(jnp.int32, (classes, LANES), 0)
    weights = jnp.zeros((classes, LANES), F32)
    for k in range(classes):
        weights = jnp.where(index == k, cw_ref[k], weights)
    cwcol[...] = weights
    for t, term in enumerate(split3(jnp.sqrt(weights))):
        at = 3 * units + t * classes
        table[at : at + classes, width : width + LANES] = term
    obs_at = 3 * (units + classes)
    tail = depth - obs_at
    obs_index = lax.broadcasted_iota(jnp.int32, (tail, LANES), 0)
    table[obs_at:, width + LANES :] = jnp.where(obs_index < 3, 1.0, 0.0).astype(BF16)
    rhs_acc[...] = jnp.zeros_like(rhs_acc)
    chi_acc[...] = jnp.zeros_like(chi_acc)
    unit_index = lax.broadcasted_iota(jnp.int32, (units, LANES), 0)

    def prepare(step):
        at = pl.multiple_of(step * LANES, LANES)
        unit_row = unit_ref[pl.ds(step, 1), :]
        class_row = class_ref[pl.ds(step, 1), :]
        obs_row = obs_ref[pl.ds(step, 1), :]
        unit_hot = jnp.where(unit_index == unit_row, 1.0, 0.0).astype(BF16)
        is_class = index == class_row
        class_hot = jnp.where(is_class, 1.0, 0.0).astype(BF16)
        row_weight = jnp.sum(jnp.where(is_class, cwcol[...], 0.0), axis=0, keepdims=True)
        chi_acc[0:1, :] += row_weight * obs_row * obs_row
        o0, o1, o2 = [t.astype(F32) for t in split3(obs_row)]
        obs_rows = jnp.where(
            obs_index == 0, o0, jnp.where(obs_index == 1, o1, jnp.where(obs_index == 2, o2, 0.0))
        ).astype(BF16)
        hot = jnp.concatenate([unit_hot] * 3 + [class_hot] * 3 + [obs_rows], axis=0)
        looked = lax.dot_general(
            hot, table[...], (((0,), (0,)), ((), ())), preferred_element_type=F32
        )
        root = looked[:, width : width + LANES]
        wobs = root * looked[:, width + LANES :]
        for b in range(width // LANES):
            cols = slice(b * LANES, (b + 1) * LANES)
            value = raw[pl.ds(at, LANES), cols].astype(F32) * (looked[:, cols] * root)
            rounded = value.astype(BF16)
            weighted[pl.ds(at, LANES), cols] = rounded
            part = (rounded.astype(F32) * wobs).reshape(LANES // 8, 8, LANES)
            rhs_acc[:, cols] += jnp.sum(part, axis=0)

    per_chunk = chunk // LANES
    for k in range(n_chunks):
        loads[k].wait()

        def body(i, carry):
            prepare(k * per_chunk + i)
            return carry

        lax.fori_loop(0, per_chunk, body, 0)

    def remote(src, dst, send, recv, device):
        return pltpu.make_async_remote_copy(
            src_ref=src, dst_ref=dst, send_sem=send, recv_sem=recv,
            device_id=device, device_id_type=MESH,
        )

    across_core = (r, y * 2 + 1 - c)
    across_x = (z * 2 + 1 - x, g)
    across_y = (r, (1 - y) * 2 + c)
    axis_of = ((across_x, x), (across_y, y))

    for b in range(width // LANES):
        axs[0, b : b + 1, :] = jnp.sum(rhs_acc[:, b * LANES : (b + 1) * LANES], axis=0, keepdims=True)
    axs[0, n_rows:, :] = jnp.broadcast_to(jnp.sum(chi_acc[0:1, :], axis=1, keepdims=True), (8, LANES))
    pl.semaphore_wait(barrier, count - 1)
    small = [remote(axs.at[0], rxa.at[0], qa.at[0], ra.at[0], across_core)]
    small[0].start()

    def small_step(k, device):
        small[k - 1].wait_recv()
        axs[k] = axs[k - 1] + rxa[k - 1]
        if device is not None:
            copy = remote(axs.at[k], rxa.at[k], qa.at[k], ra.at[k], device)
            copy.start()
            small.append(copy)

    def other_z(k):
        return lax.rem(z + k, n_z)

    def gram_panel(a):
        lo = 2 * a * LANES
        for b in range(a, n_z):
            tile = lax.dot_general(
                weighted[:, lo : lo + 2 * LANES], weighted[:, 2 * b * LANES : 2 * (b + 1) * LANES],
                (((0,), (0,)), ((), ())), preferred_element_type=F32,
            )
            for u in range(2):
                for v in range(2):
                    i, j = 2 * a + u, 2 * b + v
                    if i > j:
                        continue
                    block = tile[u * LANES : (u + 1) * LANES, v * LANES : (v + 1) * LANES]
                    if j == i + 1 and a == b:
                        for q in range(2 * n_grid):
                            dr, dg = 2 * a + q // n_grid, q % n_grid
                            for p in range(2):
                                first, second = (dr % 2, dg // 2) if p == 0 else (dg // 2, dr % 2)
                                at = q * piece + p * sub
                                buf[dr // 2, p, dg % 2, first, second, half : half + sub, :] = block[at : at + sub]
                        continue
                    if i == j or (i + j) % 2 == 1:
                        dr, dg = i, j // 2
                    else:
                        dr, dg = j, i // 2
                    for p in range(2):
                        first, second = (dr % 2, dg // 2) if p == 0 else (dg // 2, dr % 2)
                        buf[dr // 2, p, dg % 2, first, second, 0:half, :] = block[p * half : (p + 1) * half]

    def copy0(a, p):
        return remote(buf.at[a, p, 1 - c], rx0.at[a, p], q0.at[a, p], r0.at[a, p], across_core)

    def copy1(a, p):
        return remote(s1.at[a, p], rx1.at[a, p], q1.at[a, p], r1.at[a, p], axis_of[p][0])

    def copy2(a, p):
        return remote(s2.at[a, p], rx2.at[a, p], q2.at[a, p], r2.at[a, p], axis_of[1 - p][0])

    def copy3(a):
        return remote(s3.at[a], rx3.at[z], q3.at[a], r3.at[z], (a * 2 + x, g))

    def stage0(a):
        for p in range(2):
            copy0(a, p).start()

    def stage1(a):
        for p in range(2):
            first = axis_of[p][1]
            copy0(a, p).wait_recv()
            s1[a, p] = buf[a, p, c, 1 - first] + rx0[a, p, 1 - first]
            copy1(a, p).start()

    def stage2(a):
        for p in range(2):
            first, second = axis_of[p][1], axis_of[1 - p][1]
            copy1(a, p).wait_recv()
            s2[a, p] = (
                buf[a, p, c, first, 1 - second] + rx0[a, p, first, 1 - second] + rx1[a, p, 1 - second]
            )
            copy2(a, p).start()

    def stage3(a):
        for p in range(2):
            first, second = axis_of[p][1], axis_of[1 - p][1]
            copy2(a, p).wait_recv()
            s3[a, p] = (
                buf[a, p, c, first, second] + rx0[a, p, first, second] + rx1[a, p, second] + rx2[a, p]
            )

        @pl.when(z != a)
        def _():
            copy3(a).start()

    gram_panel(0)
    stage0(0)
    small_step(1, across_x)
    gram_panel(1)
    stage0(1)
    stage1(0)
    gram_panel(2)
    stage0(2)
    stage1(1)
    gram_panel(3)
    stage0(3)
    stage1(3)
    small_step(2, across_y)
    stage2(0)
    stage1(2)
    stage2(1)
    stage3(0)
    small_step(3, None)
    spread = []
    for k in range(1, n_z):
        copy = remote(
            axs.at[3], rxa.at[3 + k], qa.at[3 + k], ra.at[3 + k], (other_z(k) * 2 + x, g)
        )
        copy.start()
        spread.append(copy)
    stage2(3)
    stage3(1)
    stage2(2)
    stage3(3)
    stage3(2)

    scale = 1.0 / total_rows
    for k in range(1, n_z):
        spread[k - 1].wait_recv()
    sums = axs[3]
    for k in range(1, n_z):
        sums = sums + rxa[3 + k]
    aux_ref[...] = sums * scale

    for k in range(1, n_z):
        from_z = other_z(k)
        remote(s3.at[from_z], rx3.at[from_z], q3.at[from_z], r3.at[from_z], (from_z * 2 + x, g)).wait_recv()
    for p in range(2):
        value = s3[z, p]
        for k in range(1, n_z):
            value = value + rx3[other_z(k), p]
        value = value * scale
        fin[p * half : (p + 1) * half, :] = value[0:half]
        ext[p * sub : (p + 1) * sub, :] = value[half : half + sub]

    a = z
    mine = x * n_grid + g
    diagonal = g == a
    owned = jnp.where(g > a, 1 - x, x)
    col_owned = pl.ds(pl.multiple_of(owned * LANES, LANES), LANES)
    col_other = pl.ds(pl.multiple_of((1 - owned) * LANES, LANES), LANES)
    mirror = remote(fin, mrx, qm, rm, (2 * g + owned, a))

    @pl.when(jnp.logical_not(diagonal))
    def _():
        mirror.start()

    def extra(k):
        return remote(ext, erx.at[mine], qe.at[k], re.at[mine], (2 * a + k, a))

    for k in range(2):
        @pl.when(jnp.logical_or(jnp.logical_not(diagonal), x != k))
        def _():
            extra(k).start()

    @pl.when(g > a)
    def _():
        gram_ref[:, col_owned] = fin[...]
        mirror.wait_recv()
        gram_ref[:, col_other] = mrx[...]

    @pl.when(g < a)
    def _():
        gram_ref[:, col_owned] = fin[...].T
        mirror.wait_recv()
        gram_ref[:, col_other] = mrx[...].T

    @pl.when(diagonal)
    def _():
        gram_ref[:, col_owned] = fin[...]
        erx[mine] = ext[...]
        for k in range(1, 2 * n_grid):
            q = lax.rem(mine + k, 2 * n_grid)
            remote(ext, erx.at[q], qe.at[0], re.at[q], (2 * a + 1 - x, a)).wait_recv()
        pair = erx[...].reshape(LANES, LANES)

        @pl.when(x == 0)
        def _():
            gram_ref[:, col_other] = pair

        @pl.when(x == 1)
        def _():
            gram_ref[:, col_other] = pair.T

    for copy in small + spread:
        copy.wait_send()
    for b in range(n_z):
        for p in range(2):
            copy0(b, p).wait_send()
            copy1(b, p).wait_send()
            copy2(b, p).wait_send()

        @pl.when(z != b)
        def _():
            copy3(b).wait_send()

    @pl.when(jnp.logical_not(diagonal))
    def _():
        mirror.wait_send()

    for k in range(2):
        @pl.when(jnp.logical_or(jnp.logical_not(diagonal), x != k))
        def _():
            extra(k).wait_send()


def fused(design, observed, weight_class, calib_unit, class_weight, calib_scale):
    n_rows = lax.axis_size("rows")
    n_grid = lax.axis_size("grid")
    row_count, width = design.shape
    n_z = n_rows // 2
    units, classes = calib_scale.shape[0], class_weight.shape[0]
    piece = LANES // (2 * n_grid)
    slot = LANES // 2 + piece // 2
    depth = 3 * (units + classes) + 16
    lines = row_count // LANES
    vmem = pl.BlockSpec(memory_space=pltpu.VMEM)
    dma = pltpu.SemaphoreType.DMA
    gram, aux = pl.pallas_call(
        functools.partial(kernel, (n_rows, n_grid, row_count * n_rows * n_grid)),
        out_shape=(
            jax.ShapeDtypeStruct((LANES, 2 * LANES), F32),
            jax.ShapeDtypeStruct((n_rows + 8, LANES), F32),
        ),
        in_specs=[
            pl.BlockSpec(memory_space=pl.ANY), vmem, vmem, vmem,
            pl.BlockSpec(memory_space=pltpu.SMEM), vmem,
        ],
        out_specs=(vmem, vmem),
        scratch_shapes=[
            pltpu.VMEM((row_count, width), BF16),
            pltpu.VMEM((row_count, width), BF16),
            pltpu.VMEM((depth, width + 2 * LANES), BF16),
            pltpu.VMEM((classes, LANES), F32),
            pltpu.VMEM((8, width), F32),
            pltpu.VMEM((8, LANES), F32),
            pltpu.VMEM((n_z, 2, 2, 2, 2, slot, LANES), F32),
            pltpu.VMEM((n_z, 2, 2, 2, slot, LANES), F32),
            pltpu.VMEM((n_z, 2, 2, slot, LANES), F32),
            pltpu.VMEM((n_z, 2, 2, slot, LANES), F32),
            pltpu.VMEM((n_z, 2, slot, LANES), F32),
            pltpu.VMEM((n_z, 2, slot, LANES), F32),
            pltpu.VMEM((n_z, 2, slot, LANES), F32),
            pltpu.VMEM((n_z, 2, slot, LANES), F32),
            pltpu.VMEM((LANES, LANES), F32),
            pltpu.VMEM((piece, LANES), F32),
            pltpu.VMEM((LANES, LANES), F32),
            pltpu.VMEM((2 * n_grid, piece, LANES), F32),
            pltpu.VMEM((4, n_rows + 8, LANES), F32),
            pltpu.VMEM((3 + n_z, n_rows + 8, LANES), F32),
            dma((6,)),
            dma((n_z, 2)), dma((n_z, 2)),
            dma((n_z, 2)), dma((n_z, 2)),
            dma((n_z, 2)), dma((n_z, 2)),
            dma((n_z,)), dma((n_z,)),
            dma(()), dma(()),
            dma((2,)), dma((2 * n_grid,)),
            dma((3 + n_z,)), dma((3 + n_z,)),
        ],
        compiler_params=pltpu.CompilerParams(
            collective_id=0, has_side_effects=True, vmem_limit_bytes=60 * 1024 * 1024
        ),
    )(
        design,
        observed.reshape(lines, LANES),
        weight_class.reshape(lines, LANES),
        calib_unit.reshape(lines, LANES),
        class_weight,
        calib_scale,
    )
    part = width // (n_rows * n_grid)
    flat = (lax.axis_index("rows") * n_grid + lax.axis_index("grid")) * part
    right_hand = lax.dynamic_slice(
        aux, (flat // LANES, lax.rem(flat, LANES)), (1, part)
    ).reshape(part)
    return gram, right_hand, aux[n_rows, 0]


def local(design, observed, weight_class, calib_unit, class_weight, calib_scale):
    n_rows = lax.axis_size("rows")
    n_grid = lax.axis_size("grid")
    row_count, width = design.shape
    units, blocks = calib_scale.shape
    classes = class_weight.shape[0]
    fits = (
        n_grid == 4
        and n_rows == 8
        and width == n_rows * LANES
        and width == blocks * LANES
        and row_count % (6 * LANES) == 0
        and units % 16 == 0
        and classes % 16 == 0
    )
    run = fused if fits else plain
    return run(design, observed, weight_class, calib_unit, class_weight, calib_scale)


def solution(mesh):
    return jax.shard_map(
        local,
        mesh=mesh,
        in_specs=(
            P(("rows", "grid"), None),
            P(("rows", "grid")),
            P(("rows", "grid")),
            P(("rows", "grid")),
            P(),
            P(),
        ),
        out_specs=(P("rows", "grid"), P(("rows", "grid")), P()),
        check_vma=False,
    )
```

```python
import functools

import jax
import jax.numpy as jnp
from jax import lax
from jax.experimental import pallas as pl
from jax.experimental.pallas import tpu as pltpu
from jax.sharding import PartitionSpec as P

MESH = pl.DeviceIdType.MESH
LANES = 128
GROUP = 4
F32 = jnp.float32
BF16 = jnp.bfloat16


def plain(design, observed, weight_class, calib_unit, class_weight, calib_scale):
    row_count, width = design.shape
    blocks = calib_scale.shape[1]
    total_rows = row_count * lax.axis_size("rows") * lax.axis_size("grid")
    class_hot = (
        weight_class[:, None] == jnp.arange(class_weight.shape[0], dtype=jnp.int32)[None, :]
    ).astype(F32)
    row_weight = jnp.dot(class_hot, class_weight, precision=lax.Precision.HIGHEST)
    root_weight = jnp.sqrt(row_weight)
    unit_hot = (
        calib_unit[:, None] == jnp.arange(calib_scale.shape[0], dtype=jnp.int32)[None, :]
    ).astype(F32)
    row_scales = jnp.dot(unit_hot, calib_scale, precision=lax.Precision.HIGHEST)
    scaled = (
        (design.reshape(row_count, blocks, width // blocks).astype(F32) * row_scales[:, :, None])
        .reshape(row_count, width)
        .astype(BF16)
    )
    weighted = (root_weight[:, None] * scaled.astype(F32)).astype(BF16)
    term = lax.dot_general(weighted, weighted, (((0,), (0,)), ((), ())), preferred_element_type=F32)
    columns = lax.psum_scatter(term, "grid", scatter_dimension=1, tiled=True)
    gram = lax.psum_scatter(columns, "rows", scatter_dimension=0, tiled=True)
    weighted_obs = (root_weight * observed).astype(BF16)
    rhs_term = jnp.dot(weighted_obs, weighted, preferred_element_type=F32)
    chi_term = jnp.sum(row_weight * observed * observed)
    right_hand = lax.psum_scatter(rhs_term, ("rows", "grid"), scatter_dimension=0, tiled=True)
    chi_total = lax.psum(chi_term, ("rows", "grid"))
    return (gram / total_rows, right_hand / total_rows, chi_total / total_rows)


def split3(value):
    high = value.astype(BF16)
    rest = value - high.astype(F32)
    middle = rest.astype(BF16)
    low = (rest - middle.astype(F32)).astype(BF16)
    return high, middle, low


def kernel(
    dims,
    design_hbm, obs_ref, class_ref, unit_ref, cw_ref, cs_ref,
    gram_ref,
    raw, weighted, table, cwcol, rhs_acc, chi_acc,
    buf, rx0, s1, rx1, s2, rx2, s3, rx3, fin, ext, mrx, erx, axs, rxa,
    in_sem, q0, r0, q1, r1, q2, r2, q3, r3, qm, rm, qe, re, qa, ra,
):
    n_rows, n_grid, total_rows = dims
    n_z = n_rows // 2
    row_count, width = raw.shape
    blocks, units = cs_ref.shape
    classes = cw_ref.shape[0]
    half = LANES // 2
    piece = LANES // (2 * n_grid)
    sub = piece // 2
    r = lax.axis_index("rows")
    g = lax.axis_index("grid")
    z = r // 2
    x = lax.rem(r, 2)
    y = g // 2
    c = lax.rem(g, 2)
    me = r * n_grid + g
    count = n_rows * n_grid

    n_chunks = in_sem.shape[0]
    chunk = row_count // n_chunks
    loads = [
        pltpu.make_async_copy(
            design_hbm.at[pl.ds(k * chunk, chunk)], raw.at[pl.ds(k * chunk, chunk)], in_sem.at[k]
        )
        for k in range(n_chunks)
    ]
    for load in loads:
        load.start()

    barrier = pltpu.get_barrier_semaphore()

    def greet(k, carry):
        flat = lax.rem(me + k, count)
        pl.semaphore_signal(
            barrier, inc=1, device_id=(flat // n_grid, lax.rem(flat, n_grid)), device_id_type=MESH
        )
        return carry

    lax.fori_loop(1, count, greet, 0)

    depth = table.shape[0]
    table[...] = jnp.zeros_like(table)
    eye = lax.broadcasted_iota(jnp.int32, (units, units), 0) == lax.broadcasted_iota(
        jnp.int32, (units, units), 1
    )
    for b in range(blocks):
        square = jnp.broadcast_to(cs_ref[b : b + 1, :], (units, units))
        column = jnp.sum(jnp.where(eye, square, 0.0), axis=1, keepdims=True)
        wide = jnp.broadcast_to(column, (units, LANES))
        for t, term in enumerate(split3(wide)):
            table[t * units : (t + 1) * units, b * LANES : (b + 1) * LANES] = term
    index = lax.broadcasted_iota(jnp.int32, (classes, LANES), 0)
    weights = jnp.zeros((classes, LANES), F32)
    for k in range(classes):
        weights = jnp.where(index == k, cw_ref[k], weights)
    cwcol[...] = weights
    for t, term in enumerate(split3(jnp.sqrt(weights))):
        at = 3 * units + t * classes
        table[at : at + classes, width : width + LANES] = term
    obs_at = 3 * (units + classes)
    tail = depth - obs_at
    obs_index = lax.broadcasted_iota(jnp.int32, (tail, LANES), 0)
    table[obs_at:, width + LANES :] = jnp.where(obs_index < 3, 1.0, 0.0).astype(BF16)
    rhs_acc[...] = jnp.zeros_like(rhs_acc)
    chi_acc[...] = jnp.zeros_like(chi_acc)
    unit_index = lax.broadcasted_iota(jnp.int32, (units, LANES), 0)

    def prepare(step):
        at = pl.multiple_of(step * (GROUP * LANES), GROUP * LANES)
        hots = []
        for u in range(GROUP):
            line = pl.ds(step * GROUP + u, 1)
            unit_row, class_row, obs_row = unit_ref[line, :], class_ref[line, :], obs_ref[line, :]
            unit_hot = jnp.where(unit_index == unit_row, 1.0, 0.0).astype(BF16)
            is_class = index == class_row
            class_hot = jnp.where(is_class, 1.0, 0.0).astype(BF16)
            row_weight = jnp.sum(jnp.where(is_class, cwcol[...], 0.0), axis=0, keepdims=True)
            chi_acc[0:1, :] += row_weight * obs_row * obs_row
            o0, o1, o2 = [t.astype(F32) for t in split3(obs_row)]
            obs_rows = jnp.where(
                obs_index == 0, o0, jnp.where(obs_index == 1, o1, jnp.where(obs_index == 2, o2, 0.0))
            ).astype(BF16)
            hots.append(jnp.concatenate([unit_hot] * 3 + [class_hot] * 3 + [obs_rows], axis=0))
        hot = jnp.concatenate(hots, axis=1)
        looked = lax.dot_general(
            hot, table[...], (((0,), (0,)), ((), ())), preferred_element_type=F32
        )
        root = looked[:, width : width + LANES]
        wobs = root * looked[:, width + LANES :]
        for b in range(width // LANES):
            cols = slice(b * LANES, (b + 1) * LANES)
            value = raw[pl.ds(at, GROUP * LANES), cols].astype(F32) * (looked[:, cols] * root)
            weighted[pl.ds(at, GROUP * LANES), cols] = value.astype(BF16)
            part = (value * wobs).reshape(GROUP * LANES // 8, 8, LANES)
            rhs_acc[:, cols] += jnp.sum(part, axis=0)

    per_chunk = chunk // (GROUP * LANES)
    for k in range(n_chunks):
        loads[k].wait()

        def body(i, carry):
            prepare(k * per_chunk + i)
            return carry

        lax.fori_loop(0, per_chunk, body, 0)

    def remote(src, dst, send, recv, device):
        return pltpu.make_async_remote_copy(
            src_ref=src, dst_ref=dst, send_sem=send, recv_sem=recv,
            device_id=device, device_id_type=MESH,
        )

    across_core = (r, y * 2 + 1 - c)
    across_x = (z * 2 + 1 - x, g)
    across_y = (r, (1 - y) * 2 + c)
    axis_of = ((across_x, x), (across_y, y))

    for b in range(width // LANES):
        axs[0, b : b + 1, :] = jnp.sum(rhs_acc[:, b * LANES : (b + 1) * LANES], axis=0, keepdims=True)
    axs[0, n_rows:, :] = jnp.broadcast_to(jnp.sum(chi_acc[0:1, :], axis=1, keepdims=True), (8, LANES))
    pl.semaphore_wait(barrier, count - 1)
    small = [remote(axs.at[0], rxa.at[0], qa.at[0], ra.at[0], across_core)]
    small[0].start()

    def small_step(k, device):
        small[k - 1].wait_recv()
        axs[k] = axs[k - 1] + rxa[k - 1]
        if device is not None:
            copy = remote(axs.at[k], rxa.at[k], qa.at[k], ra.at[k], device)
            copy.start()
            small.append(copy)

    def other_z(k):
        return lax.rem(z + k, n_z)

    def gram_panel(a):
        lo = 2 * a * LANES
        for b in range(a, n_z):
            tile = lax.dot_general(
                weighted[:, lo : lo + 2 * LANES], weighted[:, 2 * b * LANES : 2 * (b + 1) * LANES],
                (((0,), (0,)), ((), ())), preferred_element_type=F32,
            )
            for u in range(2):
                for v in range(2):
                    i, j = 2 * a + u, 2 * b + v
                    if i > j:
                        continue
                    block = tile[u * LANES : (u + 1) * LANES, v * LANES : (v + 1) * LANES]
                    if j == i + 1 and a == b:
                        for q in range(2 * n_grid):
                            dr, dg = 2 * a + q // n_grid, q % n_grid
                            for p in range(2):
                                first, second = (dr % 2, dg // 2) if p == 0 else (dg // 2, dr % 2)
                                at = q * piece + p * sub
                                buf[dr // 2, p, dg % 2, first, second, half : half + sub, :] = block[at : at + sub]
                        continue
                    if i == j or (i + j) % 2 == 1:
                        dr, dg = i, j // 2
                    else:
                        dr, dg = j, i // 2
                    for p in range(2):
                        first, second = (dr % 2, dg // 2) if p == 0 else (dg // 2, dr % 2)
                        buf[dr // 2, p, dg % 2, first, second, 0:half, :] = block[p * half : (p + 1) * half]

    def copy0(a, p):
        return remote(buf.at[a, p, 1 - c], rx0.at[a, p], q0.at[a, p], r0.at[a, p], across_core)

    def copy1(a, p):
        return remote(s1.at[a, p], rx1.at[a, p], q1.at[a, p], r1.at[a, p], axis_of[p][0])

    def copy2(a, p):
        return remote(s2.at[a, p], rx2.at[a, p], q2.at[a, p], r2.at[a, p], axis_of[1 - p][0])

    def copy3(a):
        return remote(s3.at[a], rx3.at[z], q3.at[a], r3.at[z], (a * 2 + x, g))

    def stage0(a):
        for p in range(2):
            copy0(a, p).start()

    def stage1(a):
        for p in range(2):
            first = axis_of[p][1]
            copy0(a, p).wait_recv()
            s1[a, p] = buf[a, p, c, 1 - first] + rx0[a, p, 1 - first]
            copy1(a, p).start()

    def stage2(a):
        for p in range(2):
            first, second = axis_of[p][1], axis_of[1 - p][1]
            copy1(a, p).wait_recv()
            s2[a, p] = (
                buf[a, p, c, first, 1 - second] + rx0[a, p, first, 1 - second] + rx1[a, p, 1 - second]
            )
            copy2(a, p).start()

    def stage3(a):
        for p in range(2):
            first, second = axis_of[p][1], axis_of[1 - p][1]
            copy2(a, p).wait_recv()
            s3[a, p] = (
                buf[a, p, c, first, second] + rx0[a, p, first, second] + rx1[a, p, second] + rx2[a, p]
            )

        @pl.when(z != a)
        def _():
            copy3(a).start()

    gram_panel(0)
    stage0(0)
    small_step(1, across_x)
    gram_panel(1)
    stage0(1)
    stage1(0)
    gram_panel(2)
    stage0(2)
    stage1(1)
    gram_panel(3)
    stage0(3)
    stage1(3)
    small_step(2, across_y)
    stage2(0)
    stage1(2)
    stage2(1)
    stage3(0)
    small_step(3, None)
    spread = []
    for k in range(1, n_z):
        copy = remote(
            axs.at[3], rxa.at[3 + k], qa.at[3 + k], ra.at[3 + k], (other_z(k) * 2 + x, g)
        )
        copy.start()
        spread.append(copy)
    stage2(3)
    stage3(1)
    stage2(2)
    stage3(3)
    stage3(2)

    scale = 1.0 / total_rows
    for k in range(1, n_z):
        spread[k - 1].wait_recv()
    sums = axs[3]
    for k in range(1, n_z):
        sums = sums + rxa[3 + k]
    gram_ref[LANES:, 0:LANES] = sums * scale

    for k in range(1, n_z):
        from_z = other_z(k)
        remote(s3.at[from_z], rx3.at[from_z], q3.at[from_z], r3.at[from_z], (from_z * 2 + x, g)).wait_recv()
    for p in range(2):
        value = s3[z, p]
        for k in range(1, n_z):
            value = value + rx3[other_z(k), p]
        value = value * scale
        fin[p * half : (p + 1) * half, :] = value[0:half]
        ext[p * sub : (p + 1) * sub, :] = value[half : half + sub]

    a = z
    mine = x * n_grid + g
    diagonal = g == a
    owned = jnp.where(g > a, 1 - x, x)
    col_owned = pl.ds(pl.multiple_of(owned * LANES, LANES), LANES)
    col_other = pl.ds(pl.multiple_of((1 - owned) * LANES, LANES), LANES)
    mirror = remote(fin, mrx, qm, rm, (2 * g + owned, a))

    @pl.when(jnp.logical_not(diagonal))
    def _():
        mirror.start()

    def extra(k):
        return remote(ext, erx.at[mine], qe.at[k], re.at[mine], (2 * a + k, a))

    for k in range(2):
        @pl.when(jnp.logical_or(jnp.logical_not(diagonal), x != k))
        def _():
            extra(k).start()

    @pl.when(g > a)
    def _():
        gram_ref[0:LANES, col_owned] = fin[...]
        mirror.wait_recv()
        gram_ref[0:LANES, col_other] = mrx[...]

    @pl.when(g < a)
    def _():
        gram_ref[0:LANES, col_owned] = fin[...].T
        mirror.wait_recv()
        gram_ref[0:LANES, col_other] = mrx[...].T

    @pl.when(diagonal)
    def _():
        gram_ref[0:LANES, col_owned] = fin[...]
        erx[mine] = ext[...]
        for k in range(1, 2 * n_grid):
            q = lax.rem(mine + k, 2 * n_grid)
            remote(ext, erx.at[q], qe.at[0], re.at[q], (2 * a + 1 - x, a)).wait_recv()
        pair = erx[...].reshape(LANES, LANES)

        @pl.when(x == 0)
        def _():
            gram_ref[0:LANES, col_other] = pair

        @pl.when(x == 1)
        def _():
            gram_ref[0:LANES, col_other] = pair.T

    for copy in small + spread:
        copy.wait_send()
    for b in range(n_z):
        for p in range(2):
            copy0(b, p).wait_send()
            copy1(b, p).wait_send()
            copy2(b, p).wait_send()

        @pl.when(z != b)
        def _():
            copy3(b).wait_send()

    @pl.when(jnp.logical_not(diagonal))
    def _():
        mirror.wait_send()

    for k in range(2):
        @pl.when(jnp.logical_or(jnp.logical_not(diagonal), x != k))
        def _():
            extra(k).wait_send()


def finish(sums_ref, out_ref, rhs_ref, chi_ref):
    n_grid = lax.axis_size("grid")
    out_ref[...] = sums_ref[0:LANES, :]
    part = rhs_ref.shape[1]
    rows = sums_ref[LANES : LANES + 8, 0:LANES]
    index = lax.broadcasted_iota(jnp.int32, (8, LANES), 0)
    row = jnp.sum(jnp.where(index == lax.axis_index("rows"), rows, 0.0), axis=0, keepdims=True)
    turn = lax.rem(n_grid - lax.axis_index("grid"), n_grid) * part
    rhs_ref[...] = pltpu.roll(jnp.broadcast_to(row, (8, LANES)), turn, 1)[0:1, 0:part]
    chi_ref[...] = sums_ref[sums_ref.shape[0] - 8 : sums_ref.shape[0] - 7, 0:1]


def fused(design, observed, weight_class, calib_unit, class_weight, calib_scale):
    n_rows = lax.axis_size("rows")
    n_grid = lax.axis_size("grid")
    row_count, width = design.shape
    n_z = n_rows // 2
    units, classes = calib_scale.shape[0], class_weight.shape[0]
    piece = LANES // (2 * n_grid)
    slot = LANES // 2 + piece // 2
    depth = 3 * (units + classes) + 16
    lines = row_count // LANES
    vmem = pl.BlockSpec(memory_space=pltpu.VMEM)
    dma = pltpu.SemaphoreType.DMA
    sums = pl.pallas_call(
        functools.partial(kernel, (n_rows, n_grid, row_count * n_rows * n_grid)),
        out_shape=jax.ShapeDtypeStruct((LANES + n_rows + 8, 2 * LANES), F32),
        in_specs=[
            pl.BlockSpec(memory_space=pltpu.HBM), vmem, vmem, vmem,
            pl.BlockSpec(memory_space=pltpu.SMEM), vmem,
        ],
        out_specs=vmem,
        scratch_shapes=[
            pltpu.VMEM((row_count, width), BF16),
            pltpu.VMEM((row_count, width), BF16),
            pltpu.VMEM((depth, width + 2 * LANES), BF16),
            pltpu.VMEM((classes, LANES), F32),
            pltpu.VMEM((8, width), F32),
            pltpu.VMEM((8, LANES), F32),
            pltpu.VMEM((n_z, 2, 2, 2, 2, slot, LANES), F32),
            pltpu.VMEM((n_z, 2, 2, 2, slot, LANES), F32),
            pltpu.VMEM((n_z, 2, 2, slot, LANES), F32),
            pltpu.VMEM((n_z, 2, 2, slot, LANES), F32),
            pltpu.VMEM((n_z, 2, slot, LANES), F32),
            pltpu.VMEM((n_z, 2, slot, LANES), F32),
            pltpu.VMEM((n_z, 2, slot, LANES), F32),
            pltpu.VMEM((n_z, 2, slot, LANES), F32),
            pltpu.VMEM((LANES, LANES), F32),
            pltpu.VMEM((piece, LANES), F32),
            pltpu.VMEM((LANES, LANES), F32),
            pltpu.VMEM((2 * n_grid, piece, LANES), F32),
            pltpu.VMEM((4, n_rows + 8, LANES), F32),
            pltpu.VMEM((3 + n_z, n_rows + 8, LANES), F32),
            dma((6,)),
            dma((n_z, 2)), dma((n_z, 2)),
            dma((n_z, 2)), dma((n_z, 2)),
            dma((n_z, 2)), dma((n_z, 2)),
            dma((n_z,)), dma((n_z,)),
            dma(()), dma(()),
            dma((2,)), dma((2 * n_grid,)),
            dma((3 + n_z,)), dma((3 + n_z,)),
        ],
        compiler_params=pltpu.CompilerParams(
            collective_id=0, has_side_effects=True, vmem_limit_bytes=60 * 1024 * 1024
        ),
    )(
        design,
        observed.reshape(lines, LANES),
        weight_class.reshape(lines, LANES),
        calib_unit.reshape(lines, LANES),
        class_weight,
        calib_scale.T,
    )
    part = width // (n_rows * n_grid)
    gram, right_hand, chi = pl.pallas_call(
        finish,
        out_shape=(
            jax.ShapeDtypeStruct((LANES, 2 * LANES), F32),
            jax.ShapeDtypeStruct((1, part), F32),
            jax.ShapeDtypeStruct((1, 1), F32),
        ),
        in_specs=[vmem],
        out_specs=(vmem, vmem, vmem),
        compiler_params=pltpu.CompilerParams(vmem_limit_bytes=4 * 1024 * 1024),
    )(sums)
    return gram, right_hand.reshape(part), chi.reshape(())


def local(design, observed, weight_class, calib_unit, class_weight, calib_scale):
    n_rows = lax.axis_size("rows")
    n_grid = lax.axis_size("grid")
    row_count, width = design.shape
    units, blocks = calib_scale.shape
    classes = class_weight.shape[0]
    fits = (
        n_grid == 4
        and width % (n_rows * n_grid) == 0
        and n_rows == 8
        and width == n_rows * LANES
        and width == blocks * LANES
        and row_count % (6 * LANES) == 0
        and units % 16 == 0
        and classes % 16 == 0
    )
    run = fused if fits else plain
    return run(design, observed, weight_class, calib_unit, class_weight, calib_scale)


def solution(mesh):
    return jax.shard_map(
        local,
        mesh=mesh,
        in_specs=(
            P(("rows", "grid"), None),
            P(("rows", "grid")),
            P(("rows", "grid")),
            P(("rows", "grid")),
            P(),
            P(),
        ),
        out_specs=(P("rows", "grid"), P(("rows", "grid")), P()),
        check_vma=False,
    )
```

```python
import functools

import jax
import jax.numpy as jnp
from jax import lax
from jax.experimental import pallas as pl
from jax.experimental.pallas import tpu as pltpu
from jax.sharding import PartitionSpec as P

MESH = pl.DeviceIdType.MESH
LANES = 128
GROUP = 4
F32 = jnp.float32
BF16 = jnp.bfloat16


def plain(design, observed, weight_class, calib_unit, class_weight, calib_scale):
    row_count, width = design.shape
    blocks = calib_scale.shape[1]
    total_rows = row_count * lax.axis_size("rows") * lax.axis_size("grid")
    class_hot = (
        weight_class[:, None] == jnp.arange(class_weight.shape[0], dtype=jnp.int32)[None, :]
    ).astype(F32)
    row_weight = jnp.dot(class_hot, class_weight, precision=lax.Precision.HIGHEST)
    root_weight = jnp.sqrt(row_weight)
    unit_hot = (
        calib_unit[:, None] == jnp.arange(calib_scale.shape[0], dtype=jnp.int32)[None, :]
    ).astype(F32)
    row_scales = jnp.dot(unit_hot, calib_scale, precision=lax.Precision.HIGHEST)
    scaled = (
        (design.reshape(row_count, blocks, width // blocks).astype(F32) * row_scales[:, :, None])
        .reshape(row_count, width)
        .astype(BF16)
    )
    weighted = (root_weight[:, None] * scaled.astype(F32)).astype(BF16)
    term = lax.dot_general(weighted, weighted, (((0,), (0,)), ((), ())), preferred_element_type=F32)
    columns = lax.psum_scatter(term, "grid", scatter_dimension=1, tiled=True)
    gram = lax.psum_scatter(columns, "rows", scatter_dimension=0, tiled=True)
    weighted_obs = (root_weight * observed).astype(BF16)
    rhs_term = jnp.dot(weighted_obs, weighted, preferred_element_type=F32)
    chi_term = jnp.sum(row_weight * observed * observed)
    right_hand = lax.psum_scatter(rhs_term, ("rows", "grid"), scatter_dimension=0, tiled=True)
    chi_total = lax.psum(chi_term, ("rows", "grid"))
    return (gram / total_rows, right_hand / total_rows, chi_total / total_rows)


def split3(value):
    high = value.astype(BF16)
    rest = value - high.astype(F32)
    middle = rest.astype(BF16)
    low = (rest - middle.astype(F32)).astype(BF16)
    return high, middle, low


def kernel(
    dims,
    design_hbm, obs_ref, class_ref, unit_ref, cw_ref, cs_ref,
    gram_ref,
    raw, weighted, table, cwcol, rhs_acc, chi_acc,
    buf, rx0, s1, rx1, s2, rx2, s3, rx3, fin, ext, mrx, erx, axs, rxa,
    in_sem, q0, r0, q1, r1, q2, r2, q3, r3, qm, rm, qe, re, qa, ra,
):
    n_rows, n_grid, total_rows = dims
    n_z = n_rows // 2
    row_count, width = raw.shape
    blocks, units = cs_ref.shape
    classes = cw_ref.shape[0]
    half = LANES // 2
    piece = LANES // (2 * n_grid)
    sub = piece // 2
    r = lax.axis_index("rows")
    g = lax.axis_index("grid")
    z = r // 2
    x = lax.rem(r, 2)
    y = g // 2
    c = lax.rem(g, 2)
    me = r * n_grid + g
    count = n_rows * n_grid

    n_chunks = in_sem.shape[0]
    chunk = row_count // n_chunks
    loads = [
        pltpu.make_async_copy(
            design_hbm.at[pl.ds(k * chunk, chunk)], raw.at[pl.ds(k * chunk, chunk)], in_sem.at[k]
        )
        for k in range(n_chunks)
    ]
    for load in loads:
        load.start()

    barrier = pltpu.get_barrier_semaphore()

    def greet(k, carry):
        flat = lax.rem(me + k, count)
        pl.semaphore_signal(
            barrier, inc=1, device_id=(flat // n_grid, lax.rem(flat, n_grid)), device_id_type=MESH
        )
        return carry

    lax.fori_loop(1, count, greet, 0)

    depth = table.shape[0]
    table[...] = jnp.zeros_like(table)
    eye = lax.broadcasted_iota(jnp.int32, (units, units), 0) == lax.broadcasted_iota(
        jnp.int32, (units, units), 1
    )
    for b in range(blocks):
        square = jnp.broadcast_to(cs_ref[b : b + 1, :], (units, units))
        column = jnp.sum(jnp.where(eye, square, 0.0), axis=1, keepdims=True)
        wide = jnp.broadcast_to(column, (units, LANES))
        for t, term in enumerate(split3(wide)):
            table[t * units : (t + 1) * units, b * LANES : (b + 1) * LANES] = term
    index = lax.broadcasted_iota(jnp.int32, (classes, LANES), 0)
    weights = jnp.zeros((classes, LANES), F32)
    for k in range(classes):
        weights = jnp.where(index == k, cw_ref[k], weights)
    cwcol[...] = weights
    for t, term in enumerate(split3(jnp.sqrt(weights))):
        at = 3 * units + t * classes
        table[at : at + classes, width : width + LANES] = term
    obs_at = 3 * (units + classes)
    tail = depth - obs_at
    obs_index = lax.broadcasted_iota(jnp.int32, (tail, LANES), 0)
    table[obs_at:, width + LANES :] = jnp.where(obs_index < 3, 1.0, 0.0).astype(BF16)
    rhs_acc[...] = jnp.zeros_like(rhs_acc)
    chi_acc[...] = jnp.zeros_like(chi_acc)
    unit_index = lax.broadcasted_iota(jnp.int32, (units, LANES), 0)

    def prepare(step):
        at = pl.multiple_of(step * (GROUP * LANES), GROUP * LANES)
        hots = []
        for u in range(GROUP):
            line = pl.ds(step * GROUP + u, 1)
            unit_row, class_row, obs_row = unit_ref[line, :], class_ref[line, :], obs_ref[line, :]
            unit_hot = jnp.where(unit_index == unit_row, 1.0, 0.0).astype(BF16)
            is_class = index == class_row
            class_hot = jnp.where(is_class, 1.0, 0.0).astype(BF16)
            row_weight = jnp.sum(jnp.where(is_class, cwcol[...], 0.0), axis=0, keepdims=True)
            chi_acc[0:1, :] += row_weight * obs_row * obs_row
            o0, o1, o2 = [t.astype(F32) for t in split3(obs_row)]
            obs_rows = jnp.where(
                obs_index == 0, o0, jnp.where(obs_index == 1, o1, jnp.where(obs_index == 2, o2, 0.0))
            ).astype(BF16)
            hots.append(jnp.concatenate([unit_hot] * 3 + [class_hot] * 3 + [obs_rows], axis=0))
        hot = jnp.concatenate(hots, axis=1)
        looked = lax.dot_general(
            hot, table[...], (((0,), (0,)), ((), ())), preferred_element_type=F32
        )
        root = looked[:, width : width + LANES]
        wobs = root * looked[:, width + LANES :]
        for b in range(width // LANES):
            cols = slice(b * LANES, (b + 1) * LANES)
            value = raw[pl.ds(at, GROUP * LANES), cols].astype(F32) * (looked[:, cols] * root)
            weighted[pl.ds(at, GROUP * LANES), cols] = value.astype(BF16)
            part = (value * wobs).reshape(GROUP * LANES // 8, 8, LANES)
            rhs_acc[:, cols] += jnp.sum(part, axis=0)

    per_chunk = chunk // (GROUP * LANES)
    for k in range(n_chunks):
        loads[k].wait()

        def body(i, carry):
            prepare(k * per_chunk + i)
            return carry

        lax.fori_loop(0, per_chunk, body, 0)

    def remote(src, dst, send, recv, device):
        return pltpu.make_async_remote_copy(
            src_ref=src, dst_ref=dst, send_sem=send, recv_sem=recv,
            device_id=device, device_id_type=MESH,
        )

    across_core = (r, y * 2 + 1 - c)
    across_x = (z * 2 + 1 - x, g)
    across_y = (r, (1 - y) * 2 + c)
    axis_of = ((across_x, x), (across_y, y))

    for b in range(width // LANES):
        axs[0, b : b + 1, :] = jnp.sum(rhs_acc[:, b * LANES : (b + 1) * LANES], axis=0, keepdims=True)
    axs[0, n_rows:, :] = jnp.broadcast_to(jnp.sum(chi_acc[0:1, :], axis=1, keepdims=True), (8, LANES))
    pl.semaphore_wait(barrier, count - 1)
    small = [remote(axs.at[0], rxa.at[0], qa.at[0], ra.at[0], across_core)]
    small[0].start()

    def small_step(k, device):
        small[k - 1].wait_recv()
        axs[k] = axs[k - 1] + rxa[k - 1]
        if device is not None:
            copy = remote(axs.at[k], rxa.at[k], qa.at[k], ra.at[k], device)
            copy.start()
            small.append(copy)

    def other_z(k):
        return lax.rem(z + k, n_z)

    def gram_panel(a):
        lo = 2 * a * LANES
        for b in range(a, n_z):
            tile = lax.dot_general(
                weighted[:, lo : lo + 2 * LANES], weighted[:, 2 * b * LANES : 2 * (b + 1) * LANES],
                (((0,), (0,)), ((), ())), preferred_element_type=F32,
            )
            for u in range(2):
                for v in range(2):
                    i, j = 2 * a + u, 2 * b + v
                    if i > j:
                        continue
                    block = tile[u * LANES : (u + 1) * LANES, v * LANES : (v + 1) * LANES]
                    if j == i + 1 and a == b:
                        for q in range(2 * n_grid):
                            dr, dg = 2 * a + q // n_grid, q % n_grid
                            for p in range(2):
                                first, second = (dr % 2, dg // 2) if p == 0 else (dg // 2, dr % 2)
                                at = q * piece + p * sub
                                buf[dr // 2, p, dg % 2, first, second, half : half + sub, :] = block[at : at + sub]
                        continue
                    if i == j or (i + j) % 2 == 1:
                        dr, dg = i, j // 2
                    else:
                        dr, dg = j, i // 2
                    for p in range(2):
                        first, second = (dr % 2, dg // 2) if p == 0 else (dg // 2, dr % 2)
                        buf[dr // 2, p, dg % 2, first, second, 0:half, :] = block[p * half : (p + 1) * half]

    def copy0(a, p):
        return remote(buf.at[a, p, 1 - c], rx0.at[a, p], q0.at[a, p], r0.at[a, p], across_core)

    def copy1(a, p):
        return remote(s1.at[a, p], rx1.at[a, p], q1.at[a, p], r1.at[a, p], axis_of[p][0])

    def copy2(a, p):
        return remote(s2.at[a, p], rx2.at[a, p], q2.at[a, p], r2.at[a, p], axis_of[1 - p][0])

    def copy3(a):
        return remote(s3.at[a], rx3.at[z], q3.at[a], r3.at[z], (a * 2 + x, g))

    def stage0(a):
        for p in range(2):
            copy0(a, p).start()

    def stage1(a):
        for p in range(2):
            first = axis_of[p][1]
            copy0(a, p).wait_recv()
            s1[a, p] = buf[a, p, c, 1 - first] + rx0[a, p, 1 - first]
            copy1(a, p).start()

    def stage2(a):
        for p in range(2):
            first, second = axis_of[p][1], axis_of[1 - p][1]
            copy1(a, p).wait_recv()
            s2[a, p] = (
                buf[a, p, c, first, 1 - second] + rx0[a, p, first, 1 - second] + rx1[a, p, 1 - second]
            )
            copy2(a, p).start()

    def stage3(a):
        for p in range(2):
            first, second = axis_of[p][1], axis_of[1 - p][1]
            copy2(a, p).wait_recv()
            s3[a, p] = (
                buf[a, p, c, first, second] + rx0[a, p, first, second] + rx1[a, p, second] + rx2[a, p]
            )

        @pl.when(z != a)
        def _():
            copy3(a).start()

    gram_panel(0)
    stage0(0)
    small_step(1, across_x)
    gram_panel(1)
    stage0(1)
    stage1(0)
    gram_panel(2)
    stage0(2)
    stage1(1)
    gram_panel(3)
    stage0(3)
    stage1(3)
    small_step(2, across_y)
    stage2(0)
    stage1(2)
    stage2(1)
    stage2(3)
    stage3(0)
    small_step(3, None)
    spread = []
    for k in range(1, n_z):
        copy = remote(
            axs.at[3], rxa.at[3 + k], qa.at[3 + k], ra.at[3 + k], (other_z(k) * 2 + x, g)
        )
        copy.start()
        spread.append(copy)
    stage2(2)
    stage3(1)
    stage3(3)
    stage3(2)

    scale = 1.0 / total_rows
    for k in range(1, n_z):
        spread[k - 1].wait_recv()
    sums = axs[3]
    for k in range(1, n_z):
        sums = sums + rxa[3 + k]
    gram_ref[LANES:, 0:LANES] = sums * scale

    for k in range(1, n_z):
        from_z = other_z(k)
        remote(s3.at[from_z], rx3.at[from_z], q3.at[from_z], r3.at[from_z], (from_z * 2 + x, g)).wait_recv()
    for p in range(2):
        value = s3[z, p]
        for k in range(1, n_z):
            value = value + rx3[other_z(k), p]
        value = value * scale
        fin[p * half : (p + 1) * half, :] = value[0:half]
        ext[p * sub : (p + 1) * sub, :] = value[half : half + sub]

    a = z
    mine = x * n_grid + g
    diagonal = g == a
    owned = jnp.where(g > a, 1 - x, x)
    col_owned = pl.ds(pl.multiple_of(owned * LANES, LANES), LANES)
    col_other = pl.ds(pl.multiple_of((1 - owned) * LANES, LANES), LANES)
    mirror = remote(fin, mrx, qm, rm, (2 * g + owned, a))

    @pl.when(jnp.logical_not(diagonal))
    def _():
        mirror.start()

    def extra(k):
        return remote(ext, erx.at[mine], qe.at[k], re.at[mine], (2 * a + k, a))

    for k in range(2):
        @pl.when(jnp.logical_or(jnp.logical_not(diagonal), x != k))
        def _():
            extra(k).start()

    @pl.when(g > a)
    def _():
        gram_ref[0:LANES, col_owned] = fin[...]
        mirror.wait_recv()
        gram_ref[0:LANES, col_other] = mrx[...]

    @pl.when(g < a)
    def _():
        gram_ref[0:LANES, col_owned] = fin[...].T
        mirror.wait_recv()
        gram_ref[0:LANES, col_other] = mrx[...].T

    @pl.when(diagonal)
    def _():
        gram_ref[0:LANES, col_owned] = fin[...]
        erx[mine] = ext[...]
        for k in range(1, 2 * n_grid):
            q = lax.rem(mine + k, 2 * n_grid)
            remote(ext, erx.at[q], qe.at[0], re.at[q], (2 * a + 1 - x, a)).wait_recv()
        pair = erx[...].reshape(LANES, LANES)

        @pl.when(x == 0)
        def _():
            gram_ref[0:LANES, col_other] = pair

        @pl.when(x == 1)
        def _():
            gram_ref[0:LANES, col_other] = pair.T

    for copy in small + spread:
        copy.wait_send()
    for b in range(n_z):
        for p in range(2):
            copy0(b, p).wait_send()
            copy1(b, p).wait_send()
            copy2(b, p).wait_send()

        @pl.when(z != b)
        def _():
            copy3(b).wait_send()

    @pl.when(jnp.logical_not(diagonal))
    def _():
        mirror.wait_send()

    for k in range(2):
        @pl.when(jnp.logical_or(jnp.logical_not(diagonal), x != k))
        def _():
            extra(k).wait_send()


def finish(sums_ref, out_ref, rhs_ref, chi_ref):
    n_grid = lax.axis_size("grid")
    out_ref[...] = sums_ref[0:LANES, :]
    part = rhs_ref.shape[1]
    rows = sums_ref[LANES : LANES + 8, 0:LANES]
    index = lax.broadcasted_iota(jnp.int32, (8, LANES), 0)
    row = jnp.sum(jnp.where(index == lax.axis_index("rows"), rows, 0.0), axis=0, keepdims=True)
    turn = lax.rem(n_grid - lax.axis_index("grid"), n_grid) * part
    rhs_ref[...] = pltpu.roll(jnp.broadcast_to(row, (8, LANES)), turn, 1)[0:1, 0:part]
    chi_ref[...] = sums_ref[sums_ref.shape[0] - 8 : sums_ref.shape[0] - 7, 0:1]


def fused(design, observed, weight_class, calib_unit, class_weight, calib_scale):
    n_rows = lax.axis_size("rows")
    n_grid = lax.axis_size("grid")
    row_count, width = design.shape
    n_z = n_rows // 2
    units, classes = calib_scale.shape[0], class_weight.shape[0]
    piece = LANES // (2 * n_grid)
    slot = LANES // 2 + piece // 2
    depth = 3 * (units + classes) + 16
    lines = row_count // LANES
    vmem = pl.BlockSpec(memory_space=pltpu.VMEM)
    dma = pltpu.SemaphoreType.DMA
    sums = pl.pallas_call(
        functools.partial(kernel, (n_rows, n_grid, row_count * n_rows * n_grid)),
        out_shape=jax.ShapeDtypeStruct((LANES + n_rows + 8, 2 * LANES), F32),
        in_specs=[
            pl.BlockSpec(memory_space=pltpu.HBM), vmem, vmem, vmem,
            pl.BlockSpec(memory_space=pltpu.SMEM), vmem,
        ],
        out_specs=vmem,
        scratch_shapes=[
            pltpu.VMEM((row_count, width), BF16),
            pltpu.VMEM((row_count, width), BF16),
            pltpu.VMEM((depth, width + 2 * LANES), BF16),
            pltpu.VMEM((classes, LANES), F32),
            pltpu.VMEM((8, width), F32),
            pltpu.VMEM((8, LANES), F32),
            pltpu.VMEM((n_z, 2, 2, 2, 2, slot, LANES), F32),
            pltpu.VMEM((n_z, 2, 2, 2, slot, LANES), F32),
            pltpu.VMEM((n_z, 2, 2, slot, LANES), F32),
            pltpu.VMEM((n_z, 2, 2, slot, LANES), F32),
            pltpu.VMEM((n_z, 2, slot, LANES), F32),
            pltpu.VMEM((n_z, 2, slot, LANES), F32),
            pltpu.VMEM((n_z, 2, slot, LANES), F32),
            pltpu.VMEM((n_z, 2, slot, LANES), F32),
            pltpu.VMEM((LANES, LANES), F32),
            pltpu.VMEM((piece, LANES), F32),
            pltpu.VMEM((LANES, LANES), F32),
            pltpu.VMEM((2 * n_grid, piece, LANES), F32),
            pltpu.VMEM((4, n_rows + 8, LANES), F32),
            pltpu.VMEM((3 + n_z, n_rows + 8, LANES), F32),
            dma((6,)),
            dma((n_z, 2)), dma((n_z, 2)),
            dma((n_z, 2)), dma((n_z, 2)),
            dma((n_z, 2)), dma((n_z, 2)),
            dma((n_z,)), dma((n_z,)),
            dma(()), dma(()),
            dma((2,)), dma((2 * n_grid,)),
            dma((3 + n_z,)), dma((3 + n_z,)),
        ],
        compiler_params=pltpu.CompilerParams(
            collective_id=0, has_side_effects=True, vmem_limit_bytes=60 * 1024 * 1024
        ),
    )(
        design,
        observed.reshape(lines, LANES),
        weight_class.reshape(lines, LANES),
        calib_unit.reshape(lines, LANES),
        class_weight,
        calib_scale.T,
    )
    part = width // (n_rows * n_grid)
    gram, right_hand, chi = pl.pallas_call(
        finish,
        out_shape=(
            jax.ShapeDtypeStruct((LANES, 2 * LANES), F32),
            jax.ShapeDtypeStruct((1, part), F32),
            jax.ShapeDtypeStruct((1, 1), F32),
        ),
        in_specs=[vmem],
        out_specs=(vmem, vmem, vmem),
        compiler_params=pltpu.CompilerParams(vmem_limit_bytes=4 * 1024 * 1024),
    )(sums)
    return gram, right_hand.reshape(part), chi.reshape(())


def local(design, observed, weight_class, calib_unit, class_weight, calib_scale):
    n_rows = lax.axis_size("rows")
    n_grid = lax.axis_size("grid")
    row_count, width = design.shape
    units, blocks = calib_scale.shape
    classes = class_weight.shape[0]
    fits = (
        n_grid == 4
        and width % (n_rows * n_grid) == 0
        and n_rows == 8
        and width == n_rows * LANES
        and width == blocks * LANES
        and row_count % (6 * LANES) == 0
        and units % 16 == 0
        and classes % 16 == 0
    )
    run = fused if fits else plain
    return run(design, observed, weight_class, calib_unit, class_weight, calib_scale)


def solution(mesh):
    return jax.shard_map(
        local,
        mesh=mesh,
        in_specs=(
            P(("rows", "grid"), None),
            P(("rows", "grid")),
            P(("rows", "grid")),
            P(("rows", "grid")),
            P(),
            P(),
        ),
        out_specs=(P("rows", "grid"), P(("rows", "grid")), P()),
        check_vma=False,
    )
```
